32 devices in a mesh: grp: 8 (over y, x, core), mem: 4 (over z).
Axes of the slice: x: 2, y: 2, z: 4, core: 2. Of those that a mesh axis runs over, the one named last changes fastest.
Arguments:
- dyn_state: float32 [2, 58, 32, 128], P(None, None, 'grp', 'mem'), may hold values from -6 to 6
- wind_speed: float32 [58, 32, 128], P(None, 'grp', 'mem'), may hold values from -4 to 4
- mass_weight: float32 [32, 128], P('grp', 'mem'), may hold values from 0.5 to 2
- crm_state: float32 [1024, 58, 128], P(('grp', 'mem')), may hold values from -6 to 6
- batch_map: int32 [1024], P(('grp', 'mem')), may hold values from 0 to 127, as said below
- sub_steps: int32 [1024], P(('grp', 'mem')), may hold values from 1 to 2
- migrate_to: int32 [1024], P(('grp', 'mem')), may hold values from 0 to 1023, as said below
Outputs:
- dyn_next: float32 [2, 58, 32, 128], P(None, None, 'grp', 'mem')
- phys_tend: float32 [2, 58, 1024], P(None, None, ('grp', 'mem'))
- crm_next: float32 [1024, 58, 128], P(('grp', 'mem'))
The draws below stay inside these ranges and needn't reach their ends.
Inputs may be any that keep to these rules, and one draw needn't show every extreme that they name: `batch_map`: within each aligned block of 128 slots (one group), the entries are a permutation of 0 to 127. `migrate_to`: A permutation of all slots. Every slot goes to a device with the same mem index. Exactly 4 of one device's slots leave its group, at most one of them to any one other device; the rest move within the device.
All inputs are finite; a program needn't handle non-finite values.
Results may differ from the reference program's by a relative error of at most 0.0003.
Values sent between devices are 32-bit elements; how exact they have to be, the bound alone decides.
A program may use at most 64 MiB of HBM per device.

```python
import math
import jax
import jax.numpy as jnp
import numpy as np
from jax import lax

LEV = 58
CRMX = 64
NSUB = 2
EX = 8
PCOL = 32
GROUP_COLS = 128
COLUMNS = 1024
GY = 32
GX = 128
MOVES = 4
N_GRP = 8
N_MEM = 4
DEVICES = 32


def draw_batch_map(key, part):
    group_keys = jax.random.split(jax.random.fold_in(key, 11), N_GRP)
    orders = jax.vmap(lambda single_column: jax.random.permutation(single_column, GROUP_COLS))(group_keys)
    return orders.reshape(-1).astype(jnp.int32)


def draw_migrate_to(key, part):
    base = jax.random.fold_in(key, 23)

    def one_column(member):
        member_key = jax.random.fold_in(base, member)
        first_key, second_key, third_key = jax.random.split(member_key, 3)
        shifts = jax.random.permutation(first_key, N_GRP - 1)[:MOVES] + 1
        chosen = jax.random.permutation(second_key, PCOL)[:MOVES]
        shift_of_slot = jnp.zeros((PCOL,), jnp.int32).at[chosen].set(shifts.astype(jnp.int32))
        group_index = jnp.arange(N_GRP, dtype=jnp.int32)[:, None]
        dest_group = (group_index + shift_of_slot[None, :]) % N_GRP
        orders = jax.vmap(lambda single_column: jax.random.permutation(single_column, PCOL))(jax.random.split(third_key, N_GRP)).astype(jnp.int32)
        slot_index = jnp.broadcast_to(jnp.arange(PCOL, dtype=jnp.int32)[None, :], (N_GRP, PCOL))
        dest_slot = orders[dest_group, slot_index]
        return (dest_group * N_MEM + member) * PCOL + dest_slot
    every = jax.vmap(one_column)(jnp.arange(N_MEM, dtype=jnp.int32))
    return every.transpose(1, 0, 2).reshape(-1).astype(jnp.int32)


def with_ends(values, stream_key, low, top_value):
    dims = values.shape
    index_at = [jax.random.randint(jax.random.fold_in(stream_key, axis), (), 0, dims[axis]) for axis in range(len(dims))]
    values = values.at[tuple(index_at)].set(low)
    longest = dims.index(max(dims))
    index_at[longest] = (index_at[longest] + 1) % dims[longest]
    return values.at[tuple(index_at)].set(top_value)


def block_scale(own_key, extent, cuts, low, largest):
    gain, own = 1.0, jax.random.fold_in(own_key, 6)
    for dim, blocks in cuts:
        heights = jnp.exp(jax.random.uniform(jax.random.fold_in(own, dim), (blocks,), jnp.float32, low / len(cuts), largest / len(cuts)))
        gain = gain * jnp.repeat(heights, extent[dim] // blocks).reshape([-1 if axis == dim else 1 for axis in range(len(extent))])
    return gain


def scatter_about(key, shape, scale, reach, pieces=(), kind=jnp.bfloat16):
    values = scale * jax.random.normal(key, shape, jnp.float32)
    if pieces:
        values = values * block_scale(key, shape, pieces, -0.22, 0.18)
    return jnp.clip(values, -reach, reach).astype(kind)


def setup_inputs(seed: int = 0) -> dict:
    key_of = jax.random.split(jax.random.key(seed), 8)
    dyn_state = scatter_about(key_of[0], (2, LEV, GY, GX), 1.0, 6.0, ((2, 8), (3, 4)), jnp.float32)
    wind_speed = scatter_about(key_of[1], (LEV, GY, GX), 1.0, 4.0, ((1, 8), (2, 4)), jnp.float32)
    mass_weight = jnp.clip(jnp.exp(math.log(2.0) - 1.3862944 * jax.random.uniform(key_of[2], (GY, GX), jnp.float32) ** block_scale(key_of[2], (GY, GX), ((0, 8), (1, 4)), -0.2, 0.2)), 0.5, 2.0)
    crm_state = scatter_about(key_of[3], (COLUMNS, LEV, 2 * CRMX), 1.0, 6.0, ((0, 32),), jnp.float32)
    batch_map = draw_batch_map(jax.random.fold_in(key_of[7], 71), 0)
    sub_steps = with_ends(jax.random.randint(key_of[5], (COLUMNS,), 1, NSUB + 1), jax.random.fold_in(key_of[5], 1), 1, NSUB).astype(jnp.int32)
    migrate_to = draw_migrate_to(jax.random.fold_in(key_of[7], 71), 0)
    return {"dyn_state": dyn_state, "wind_speed": wind_speed, "mass_weight": mass_weight, "crm_state": crm_state, "batch_map": batch_map, "sub_steps": sub_steps, "migrate_to": migrate_to}


def derivative_table():
    nodes = np.array([-1.0, -1.0 / np.sqrt(5.0), 1.0 / np.sqrt(5.0), 1.0])
    table = np.zeros((4, 4))
    for target_node in range(4):
        for source_node in range(4):
            if target_node == source_node:
                table[target_node, source_node] = sum((1.0 / (nodes[source_node] - nodes[other_node]) for other_node in range(4) if other_node != source_node))
            else:
                numerator = 1.0
                for other_node in range(4):
                    if other_node != source_node and other_node != target_node:
                        numerator = numerator * (nodes[target_node] - nodes[other_node])
                denominator = 1.0
                for other_node in range(4):
                    if other_node != source_node:
                        denominator = denominator * (nodes[source_node] - nodes[other_node])
                table[target_node, source_node] = numerator / denominator
    return table.astype(np.float32)

def element_derivative(field):
    shape_in = field.shape
    blocks = field.reshape(shape_in[:-1] + (shape_in[-1] // 4, 4))
    table = jnp.asarray(derivative_table()).astype(field.dtype)
    result = jnp.einsum('...ej,ij->...ei', blocks, table, precision=lax.Precision.HIGHEST)
    return result.reshape(shape_in)

def assemble_axis(values, axis):
    length = values.shape[axis]
    shape_b = [1] * values.ndim
    shape_b[axis] = length
    position = jnp.arange(length, dtype=jnp.int32)
    opening = (position % 4 == 0).reshape(shape_b)
    closing = (position % 4 == 3).reshape(shape_b)
    return values + jnp.where(opening, jnp.roll(values, 1, axis), 0.0) + jnp.where(closing, jnp.roll(values, -1, axis), 0.0)

def second_levels(values):
    upper = jnp.concatenate([values[:, 1:], values[:, -1:]], 1)
    lower = jnp.concatenate([values[:, :1], values[:, :-1]], 1)
    return upper + lower - 2.0 * values

def second_columns(values):
    return jnp.roll(values, 1, -1) + jnp.roll(values, -1, -1) - 2.0 * values

def crm_run(state, forcing, steps):
    width = state.shape[-1] // 2
    force_heat = forcing[0].T[:, :, None]
    force_moist = forcing[1].T[:, :, None]
    thermal = state[..., :width]
    moisture = state[..., width:]
    for substep in range(NSUB):
        condense = 0.1 * jax.nn.softplus(moisture - thermal)
        thermal_new = thermal + 0.25 * force_heat + 0.15 * second_columns(thermal) + 0.1 * second_levels(thermal) + 0.5 * condense
        moisture_new = moisture + 0.25 * force_moist + 0.15 * second_columns(moisture) + 0.1 * second_levels(moisture) - condense
        active = (steps > substep)[:, None, None]
        thermal = jnp.where(active, thermal_new, thermal)
        moisture = jnp.where(active, moisture_new, moisture)
    final = jnp.concatenate([thermal, moisture], -1)
    tendency = jnp.stack([lax.optimization_barrier(jnp.mean(thermal - state[..., :width], -1)).T, lax.optimization_barrier(jnp.mean(moisture - state[..., width:], -1)).T])
    return (final, tendency)

def reference(dyn_state, wind_speed, mass_weight, crm_state, batch_map, sub_steps, migrate_to):
    advection = -wind_speed[None] * element_derivative(dyn_state)
    numerator = assemble_axis(assemble_axis(mass_weight[None, None] * advection, 3), 2)
    denominator = assemble_axis(assemble_axis(mass_weight, 1), 0)
    assembled = numerator / denominator
    dyn_next = dyn_state + 0.2 * assembled
    levels = dyn_state.shape[1]
    blocked = assembled.reshape(2, levels, GY // 2, 2, GX // 2, 2).mean((3, 5))
    blocked = blocked.reshape(2, levels, N_GRP, 2, N_MEM, 2 * EX).transpose(0, 1, 2, 4, 3, 5)
    forcing = blocked.reshape(2, levels, COLUMNS)
    group_base = jnp.arange(COLUMNS, dtype=jnp.int32) // GROUP_COLS * GROUP_COLS
    source = (group_base + batch_map).astype(jnp.int32)
    forcing_position = forcing[:, :, source]
    state_blocks = crm_state.reshape(DEVICES, PCOL, levels, crm_state.shape[-1])
    force_blocks = forcing_position.reshape(2, levels, DEVICES, PCOL).transpose(2, 0, 1, 3)
    step_blocks = sub_steps.reshape(DEVICES, PCOL)

    def per_device(bundle):
        return crm_run(bundle[0], bundle[1], bundle[2])
    stepped, tendency_blocks = lax.map(per_device, (state_blocks, force_blocks, step_blocks))
    stepped = stepped.reshape(crm_state.shape)
    tendency_slot = tendency_blocks.transpose(1, 2, 0, 3).reshape(2, levels, COLUMNS)
    phys_tend = jnp.zeros((2, levels, COLUMNS), jnp.float32).at[:, :, source].set(tendency_slot)
    crm_next = jnp.zeros_like(stepped).at[migrate_to.astype(jnp.int32)].set(stepped)
    return (dyn_next, phys_tend, crm_next)
```

```python
import functools

import jax
import jax.numpy as jnp
import numpy as np
from jax import lax
from jax.experimental import pallas as pl
from jax.experimental.pallas import tpu as pltpu
from jax.sharding import PartitionSpec as P

NSUB = 2
MESH = pl.DeviceIdType.MESH
F32 = jnp.float32
BF16 = jnp.bfloat16
LANES = 128


def derivative_table():
    nodes = np.array([-1.0, -1.0 / np.sqrt(5.0), 1.0 / np.sqrt(5.0), 1.0])
    table = np.zeros((4, 4))
    for i in range(4):
        for j in range(4):
            if i == j:
                table[i, j] = sum(1.0 / (nodes[j] - nodes[o]) for o in range(4) if o != j)
            else:
                top, bottom = 1.0, 1.0
                for o in range(4):
                    if o != j and o != i:
                        top = top * (nodes[i] - nodes[o])
                    if o != j:
                        bottom = bottom * (nodes[j] - nodes[o])
                table[i, j] = top / bottom
    return table.astype(np.float32)


def split(values):
    high = values.astype(BF16)
    low = (values - high.astype(F32)).astype(BF16)
    return jnp.concatenate([high, low], axis=-1)


def explicit_part(cur, width):
    lane = lax.broadcasted_iota(jnp.int32, cur.shape, 1)
    heat = lane < width
    inner = lane % width
    other = pltpu.roll(cur, width, 1)
    diff = other - cur
    gap = jnp.where(heat, diff, -diff)
    condense = jnp.maximum(gap, 0.0) + jnp.log(1.0 + jnp.exp(-jnp.abs(gap)))
    left = jnp.where(inner == 0, pltpu.roll(cur, width + 1, 1), pltpu.roll(cur, 1, 1))
    right = jnp.where(
        inner == width - 1,
        pltpu.roll(cur, width - 1, 1),
        pltpu.roll(cur, 2 * width - 1, 1),
    )
    upper = jnp.concatenate([cur[1:], cur[-1:]], 0)
    lower = jnp.concatenate([cur[:1], cur[:-1]], 0)
    scale = jnp.where(heat, 0.05, -0.1)
    return 0.5 * cur + 0.15 * (left + right) + 0.1 * (upper + lower) + scale * condense


def exchange(n_grp, n_mem, levels, rows, points, slots, width, *refs):
    (dyn_ref, wind_ref, mass_ref, crm_hbm, bmap_ref, steps_ref, migrate_ref,
     deriv_ref, spread_ref, pick_ref,
     asm_ref, phys_ref, stepped_ref, arrived_ref,
     crm, part0, vt, vrow, edge_s, edge_x, edge_y_s, edge_y, edge_d_s, edge_d,
     pair, own_f, gathered, fslot, bucket, tend, outgoing, incoming,
     crm_sem, sx_sem, rx_sem, sy_sem, ry_sem, sd_sem, rd_sem,
     sg_sem, rg_sem, sb_sem, rb_sem, st_sem, rt_sem) = refs
    g, m = lax.axis_index("grp"), lax.axis_index("mem")
    fields = 2 * levels

    load = pltpu.make_async_copy(crm_hbm, crm, crm_sem)
    load.start()

    gu, gd = lax.rem(g + n_grp - 1, n_grp), lax.rem(g + 1, n_grp)
    ml, mr = lax.rem(m + n_mem - 1, n_mem), lax.rem(m + 1, n_mem)
    corners = ((gd, mr), (gd, ml), (gu, mr), (gu, ml))
    barrier = pltpu.get_barrier_semaphore()
    for o in range(1, n_grp):
        pl.semaphore_signal(barrier, 1, device_id=(lax.rem(g + o, n_grp), m), device_id_type=MESH)
    for o in range(1, n_mem):
        pl.semaphore_signal(barrier, 1, device_id=(g, lax.rem(m + o, n_mem)), device_id_type=MESH)
    for corner in corners:
        pl.semaphore_signal(barrier, 1, device_id=corner, device_id_type=MESH)

    deriv = deriv_ref[...]
    for r in range(rows):
        mass = mass_ref[r:r + 1, :]
        wind = wind_ref[pl.ds(r, levels, stride=rows), :]
        factor = -wind * mass
        for f in range(2):
            x = dyn_ref[pl.ds(f * levels * rows + r, levels, stride=rows), :]
            dx = jnp.dot(x, deriv, precision=lax.Precision.HIGHEST, preferred_element_type=F32)
            vrow[pl.ds(f * levels, levels), :] = factor * dx
        vrow[pl.ds(fields, LANES - fields), :] = jnp.broadcast_to(mass, (LANES - fields, points))
        value = vrow[...].T
        vt[r] = value
        edge_s[0, r:r + 1, :] = value[points - 1:, :]
        edge_s[1, r:r + 1, :] = value[:1, :]
        if r == rows - 1:
            edge_y_s[0] = value
            edge_d_s[0, 0:1, :] = value[points - 1:, :]
            edge_d_s[1, 0:1, :] = value[:1, :]
        if r == 0:
            edge_y_s[1] = value
            edge_d_s[2, 0:1, :] = value[points - 1:, :]
            edge_d_s[3, 0:1, :] = value[:1, :]

    pl.semaphore_wait(barrier, n_grp - 1 + n_mem - 1 + 4)

    def remote(src, dst, ssem, rsem, device):
        return pltpu.make_async_remote_copy(
            src_ref=src, dst_ref=dst, send_sem=ssem, recv_sem=rsem,
            device_id=device, device_id_type=MESH)

    halos = []
    for i, corner in enumerate(corners):
        halos.append(remote(edge_d_s.at[i], edge_d.at[i], sd_sem.at[i], rd_sem.at[i], corner))
    for i, near in enumerate((gd, gu)):
        halos.append(remote(edge_y_s.at[i], edge_y.at[i], sy_sem.at[i], ry_sem.at[i], (near, m)))
    for i, near in enumerate((mr, ml)):
        halos.append(remote(edge_s.at[i], edge_x.at[i], sx_sem.at[i], rx_sem.at[i], (g, near)))
    for copy in halos:
        copy.start()

    load.wait()

    def first(s, carry):
        part0[s] = explicit_part(crm[s], width)
        return carry

    lax.fori_loop(0, slots, first, 0, unroll=2)

    for copy in halos:
        copy.wait()

    position = lax.broadcasted_iota(jnp.int32, (points, LANES), 0)

    def sweep(value, before, after):
        lower = jnp.where(position == 0, before, pltpu.roll(value, 1, 0))
        upper = jnp.where(position == points - 1, after, pltpu.roll(value, points - 1, 0))
        return (value + jnp.where(position % 4 == 0, lower, 0.0)
                + jnp.where(position % 4 == 3, upper, 0.0))

    swept = [sweep(edge_y[0], edge_d[0, 0:1, :], edge_d[1, 0:1, :])]
    for r in range(rows):
        swept.append(sweep(vt[r], edge_x[0, r:r + 1, :], edge_x[1, r:r + 1, :]))
    swept.append(sweep(edge_y[1], edge_d[2, 0:1, :], edge_d[3, 0:1, :]))
    results = []
    for r in range(rows):
        total = swept[r + 1]
        if r % 4 == 0:
            total = total + swept[r]
        if r % 4 == 3:
            total = total + swept[r + 2]
        result = total / total[:, fields:fields + 1]
        asm_ref[r] = result
        results.append(result)
    half = points // 2
    for b in range(rows // 2):
        pair[...] = 0.25 * (results[2 * b] + results[2 * b + 1])
        own_f[pl.ds(b * half, half), :] = (
            pair[pl.ds(0, half, stride=2), :] + pair[pl.ds(1, half, stride=2), :])

    here = pl.ds(pl.multiple_of(m * slots, slots), slots)
    sends = [
        remote(own_f, gathered.at[o - 1], sg_sem.at[o - 1], rg_sem.at[o - 1],
               (g, lax.rem(m + o, n_mem)))
        for o in range(1, n_mem)]
    for copy in sends:
        copy.start()
    cols = lax.broadcasted_iota(jnp.int32, (slots, slots), 1)
    served = bmap_ref[...]

    def place(source):
        mine = (served == cols + source * slots).astype(BF16)
        return mine

    total = jnp.dot(place(m), split(own_f[...]), preferred_element_type=F32)
    for o in range(1, n_mem):
        sends[o - 1].wait()
        total = total + jnp.dot(place(lax.rem(m + n_mem - o, n_mem)), split(gathered[o - 1]),
                                preferred_element_type=F32)
    fslot[...] = total

    def second(index):
        row = fslot[pl.ds(index, 1), :]
        chosen = (pick_ref[...] * row).astype(BF16)
        forced = 0.25 * jnp.dot(chosen, spread_ref[:, :LANES], preferred_element_type=F32)[:levels]
        start = crm[index]
        count = steps_ref[index]
        cur = jnp.where(count > 0, part0[index] + forced, start)
        cur = jnp.where(count > 1, explicit_part(cur, width) + forced, cur)
        return cur, start

    span = n_mem * slots

    def leave(i, carry):
        target = lax.rem(g + i + 1, n_grp)
        low = target * span + m * slots
        index, mark = jnp.int32(0), jnp.int32(0)
        for s in range(slots):
            where_to = migrate_ref[s]
            hit = (where_to >= low) & (where_to < low + slots)
            index = jnp.where(hit, s, index)
            mark = jnp.where(hit, where_to - low + 1, mark)
        cur, _ = second(index)
        bucket[i, 0:levels, :] = cur
        bucket[i, levels:, :] = jnp.full((bucket.shape[1] - levels, LANES), mark.astype(F32))
        remote(bucket.at[i], arrived_ref.at[i], sb_sem.at[i], rb_sem.at[i], (target, m)).start()
        return carry

    lax.fori_loop(0, n_grp - 1, leave, 0)

    def stay(s, carry):
        cur, start = second(s)
        stepped_ref[s] = cur
        change = jnp.dot(split(cur - start), spread_ref[:, LANES:], preferred_element_type=F32)
        chosen = jnp.where(pick_ref[0:levels, 0:LANES] > 0.0, change, 0.0)
        tend[pl.ds(s, 1), :] = jnp.sum(chosen, 0, keepdims=True) * (1.0 / width)
        return carry

    lax.fori_loop(0, slots, stay, 0, unroll=2)

    def route(dest):
        mine = (served == cols + dest * slots).astype(F32)
        return lax.dot_general(mine, tend[...], (((0,), (0,)), ((), ())),
                               precision=lax.Precision.HIGHEST, preferred_element_type=F32)

    returns = []
    for o in range(1, n_mem):
        dest = lax.rem(m + o, n_mem)
        outgoing[o - 1] = route(dest)
        copy = remote(outgoing.at[o - 1], incoming.at[o - 1], st_sem.at[o - 1], rt_sem.at[o - 1],
                      (g, dest))
        copy.start()
        returns.append(copy)
    sums = route(m)
    for o in range(1, n_mem):
        returns[o - 1].wait()
        sums = sums + incoming[o - 1]
    phys_ref[...] = sums

    def finish(i, carry):
        target = lax.rem(g + i + 1, n_grp)
        remote(bucket.at[i], arrived_ref.at[i], sb_sem.at[i], rb_sem.at[i], (target, m)).wait()
        return carry

    lax.fori_loop(0, n_grp - 1, finish, 0)


def place_outputs(n_grp, n_mem, levels, rows, points, slots, *refs):
    (migrate_ref, dyn_ref, asm_ref, phys_ref, stepped_ref, arrived_ref,
     dyn_out, phys_out, crm_out) = refs
    g = lax.axis_index("grp")
    fields = 2 * levels
    span = n_mem * slots
    low = g * span
    for s in range(slots):
        where_to = migrate_ref[s]

        @pl.when((where_to >= low) & (where_to < low + span))
        def _():
            crm_out[lax.rem(where_to, slots)] = stepped_ref[s]

    for r in range(rows):
        back = asm_ref[r].T
        at = pl.ds(r, fields, stride=rows)
        dyn_out[at, :] = dyn_ref[at, :] + 0.2 * back[:fields]
    turned = phys_ref[...].T
    phys_out[0] = turned[:levels]
    phys_out[1] = turned[levels:fields]

    def settle(i, carry):
        mark = jnp.max(arrived_ref[i, levels:levels + 1, :]).astype(jnp.int32)

        @pl.when(mark > 0)
        def _():
            crm_out[mark - 1] = arrived_ref[i, 0:levels, :]

        return carry

    lax.fori_loop(0, n_grp - 1, settle, 0)


def on_device(n_grp, n_mem, dyn_state, wind_speed, mass_weight, crm_state, batch_map, sub_steps,
              migrate_to):
    _, levels, rows, points = dyn_state.shape
    slots = crm_state.shape[0]
    width = crm_state.shape[2] // 2
    fields = 2 * levels
    padded = levels // 8 * 8 + 8
    deriv = np.kron(np.eye(points // 4), derivative_table().T).astype(np.float32)
    k = np.arange(LANES)
    half_of_k = np.where(k < fields, k // levels, 2)
    half_of_x = np.arange(2 * width) // width
    same = (half_of_k[:, None] == half_of_x[None, :]).astype(np.float32)
    spread = np.concatenate([np.tile(same, (2, 1)), np.tile(same.T, (2, 1))], 1)
    pick = ((k[None, :] % levels == np.arange(padded)[:, None]) & (k[None, :] < fields))
    pick = np.tile(pick.astype(np.float32), (1, 2))
    dyn2 = dyn_state.reshape(fields * rows, points)
    wind2 = wind_speed.reshape(levels * rows, points)
    vmem = pl.BlockSpec(memory_space=pltpu.VMEM)
    smem = pl.BlockSpec(memory_space=pltpu.SMEM)
    hbm = pl.BlockSpec(memory_space=pl.ANY)
    dma = pltpu.SemaphoreType.DMA
    sds = jax.ShapeDtypeStruct
    asm, phys, stepped, arrived = pl.pallas_call(
        functools.partial(exchange, n_grp, n_mem, levels, rows, points, slots, width),
        out_shape=(
            sds((rows, points, LANES), F32),
            sds((slots, LANES), F32),
            sds((slots, levels, 2 * width), F32),
            sds((n_grp - 1, padded, LANES), F32),
        ),
        in_specs=[vmem, vmem, vmem, hbm, vmem, smem, smem, vmem, vmem, vmem],
        out_specs=(vmem, vmem, vmem, hbm),
        scratch_shapes=[
            pltpu.VMEM((slots, levels, 2 * width), F32),
            pltpu.VMEM((slots, levels, 2 * width), F32),
            pltpu.VMEM((rows, points, LANES), F32),
            pltpu.VMEM((LANES, points), F32),
            pltpu.VMEM((2, 8, LANES), F32),
            pltpu.VMEM((2, 8, LANES), F32),
            pltpu.VMEM((2, points, LANES), F32),
            pltpu.VMEM((2, points, LANES), F32),
            pltpu.VMEM((4, 8, LANES), F32),
            pltpu.VMEM((4, 8, LANES), F32),
            pltpu.VMEM((points, LANES), F32),
            pltpu.VMEM((slots, LANES), F32),
            pltpu.VMEM((n_mem - 1, slots, LANES), F32),
            pltpu.VMEM((slots, 2 * LANES), F32),
            pltpu.VMEM((n_grp - 1, padded, LANES), F32),
            pltpu.VMEM((slots, LANES), F32),
            pltpu.VMEM((n_mem - 1, slots, LANES), F32),
            pltpu.VMEM((n_mem - 1, slots, LANES), F32),
            dma,
            dma((2,)), dma((2,)), dma((2,)), dma((2,)), dma((4,)), dma((4,)),
            dma((n_mem - 1,)), dma((n_mem - 1,)),
            dma((n_grp - 1,)), dma((n_grp - 1,)),
            dma((n_mem - 1,)), dma((n_mem - 1,)),
        ],
        compiler_params=pltpu.CompilerParams(collective_id=0, has_side_effects=True),
        name="exchange",
    )(dyn2, wind2, mass_weight, crm_state, batch_map[:, None], sub_steps, migrate_to,
      jnp.asarray(deriv), jnp.asarray(spread).astype(BF16), jnp.asarray(pick))
    dyn_next, phys_tend, crm_next = pl.pallas_call(
        functools.partial(place_outputs, n_grp, n_mem, levels, rows, points, slots),
        out_shape=(
            sds((fields * rows, points), F32),
            sds((2, levels, slots), F32),
            sds((slots, levels, 2 * width), F32),
        ),
        in_specs=[smem, vmem, vmem, vmem, vmem, vmem],
        out_specs=(vmem, vmem, vmem),
        name="place",
    )(migrate_to, dyn2, asm, phys, stepped, arrived)
    return dyn_next.reshape(dyn_state.shape), phys_tend, crm_next


def solution(mesh):
    n_grp, n_mem = mesh.shape["grp"], mesh.shape["mem"]
    grid = P(None, None, "grp", "mem")
    slot = P(("grp", "mem"))
    return jax.shard_map(
        functools.partial(on_device, n_grp, n_mem),
        mesh=mesh,
        in_specs=(grid, P(None, "grp", "mem"), P("grp", "mem"), P(("grp", "mem"), None, None),
                  slot, slot, slot),
        out_specs=(grid, P(None, None, ("grp", "mem")), P(("grp", "mem"), None, None)),
        check_vma=False,
    )
```

```python
import functools

import jax
import jax.numpy as jnp
import numpy as np
from jax import lax
from jax.experimental import pallas as pl
from jax.experimental.pallas import tpu as pltpu
from jax.sharding import PartitionSpec as P

NSUB = 2
MESH = pl.DeviceIdType.MESH
F32 = jnp.float32
BF16 = jnp.bfloat16
LANES = 128
UNROLL = 8


def derivative_table():
    nodes = np.array([-1.0, -1.0 / np.sqrt(5.0), 1.0 / np.sqrt(5.0), 1.0])
    table = np.zeros((4, 4))
    for i in range(4):
        for j in range(4):
            if i == j:
                table[i, j] = sum(1.0 / (nodes[j] - nodes[o]) for o in range(4) if o != j)
            else:
                top, bottom = 1.0, 1.0
                for o in range(4):
                    if o != j and o != i:
                        top = top * (nodes[i] - nodes[o])
                    if o != j:
                        bottom = bottom * (nodes[j] - nodes[o])
                table[i, j] = top / bottom
    return table.astype(np.float32)


def split(values):
    high = values.astype(BF16)
    low = (values - high.astype(F32)).astype(BF16)
    return jnp.concatenate([high, low], axis=-1)


def half_steps(cur, upper, lower, width):
    lane = lax.broadcasted_iota(jnp.int32, cur.shape, 1)
    heat = lane < width
    inner = lane % width
    other = pltpu.roll(cur, width, 1)
    diff = other - cur
    gap = jnp.where(heat, diff, -diff)
    condense = jnp.maximum(gap, 0.0) + jnp.log(1.0 + jnp.exp(-jnp.abs(gap)))
    left = jnp.where(inner == 0, pltpu.roll(cur, width + 1, 1), pltpu.roll(cur, 1, 1))
    right = jnp.where(
        inner == width - 1,
        pltpu.roll(cur, width - 1, 1),
        pltpu.roll(cur, 2 * width - 1, 1),
    )
    scale = jnp.where(heat, 0.05, -0.1)
    return 0.5 * cur + 0.15 * (left + right) + 0.1 * (upper + lower) + scale * condense


def blocks(levels, unroll, body, carry):
    full = levels // unroll
    if full:
        carry = lax.fori_loop(0, full, lambda i, c: body(i * unroll, unroll, c), carry)
    if levels % unroll:
        carry = body(full * unroll, levels % unroll, carry)
    return carry


def exchange(n_grp, n_mem, levels, rows, points, slots, width, *refs):
    (dyn_ref, wind_ref, mass_ref, crm_hbm, bmap_ref, steps_ref, migrate_ref,
     deriv_ref, same_ref,
     asm_ref, phys_ref, stepped_ref, arrived_ref,
     crm, part, mid, xs, ws, edge_s, edge_x, edge_y_s, edge_y, edge_d_s, edge_d,
     pair, own_f, gathered, bucket, tend, outgoing, incoming, index_s, mark_s,
     crm_sem, sx_sem, rx_sem, sy_sem, ry_sem, sd_sem, rd_sem,
     sg_sem, rg_sem, sb_sem, rb_sem, st_sem, rt_sem) = refs
    g, m = lax.axis_index("grp"), lax.axis_index("mem")
    fields = 2 * levels
    span = n_mem * slots

    load = pltpu.make_async_copy(crm_hbm, crm, crm_sem)
    load.start()

    gu, gd = lax.rem(g + n_grp - 1, n_grp), lax.rem(g + 1, n_grp)
    ml, mr = lax.rem(m + n_mem - 1, n_mem), lax.rem(m + 1, n_mem)
    corners = ((gd, mr), (gd, ml), (gu, mr), (gu, ml))
    barrier = pltpu.get_barrier_semaphore()
    for o in range(1, n_grp):
        pl.semaphore_signal(barrier, 1, device_id=(lax.rem(g + o, n_grp), m), device_id_type=MESH)
    for o in range(1, n_mem):
        pl.semaphore_signal(barrier, 1, device_id=(g, lax.rem(m + o, n_mem)), device_id_type=MESH)
    for corner in corners:
        pl.semaphore_signal(barrier, 1, device_id=corner, device_id_type=MESH)

    for r in range(rows):
        at = pl.ds(r * points, points)
        for f in range(2):
            xs[at, f * levels:(f + 1) * levels] = dyn_ref[f, r]
            ws[at, f * levels:(f + 1) * levels] = wind_ref[r]
        spread_mass = jnp.broadcast_to(mass_ref[r:r + 1, :], (LANES, points)).T
        xs[at, fields:] = jnp.zeros((points, LANES - fields), F32)
        ws[at, fields:] = -spread_mass[:, fields:]
    lane = lax.broadcasted_iota(jnp.int32, (points, LANES), 1)
    values = []
    dx = jnp.dot(deriv_ref[...], xs[...], precision=lax.Precision.HIGHEST,
                 preferred_element_type=F32)
    for r in range(rows):
        at = slice(r * points, (r + 1) * points)
        spread_mass = jnp.broadcast_to(mass_ref[r:r + 1, :], (LANES, points)).T
        advected = -ws[at] * jnp.where(lane < fields, dx[at] * spread_mass, 1.0)
        values.append(advected)
        edge_s[0, r:r + 1, :] = advected[points - 1:, :]
        edge_s[1, r:r + 1, :] = advected[:1, :]
        if r == rows - 1:
            edge_y_s[0] = advected
            edge_d_s[0, 0:1, :] = advected[points - 1:, :]
            edge_d_s[1, 0:1, :] = advected[:1, :]
        if r == 0:
            edge_y_s[1] = advected
            edge_d_s[2, 0:1, :] = advected[points - 1:, :]
            edge_d_s[3, 0:1, :] = advected[:1, :]

    pl.semaphore_wait(barrier, n_grp - 1 + n_mem - 1 + 4)

    def remote(src, dst, ssem, rsem, device):
        return pltpu.make_async_remote_copy(
            src_ref=src, dst_ref=dst, send_sem=ssem, recv_sem=rsem,
            device_id=device, device_id_type=MESH)

    halos = []
    for i, corner in enumerate(corners):
        halos.append(remote(edge_d_s.at[i], edge_d.at[i], sd_sem.at[i], rd_sem.at[i], corner))
    for i, near in enumerate((gd, gu)):
        halos.append(remote(edge_y_s.at[i], edge_y.at[i], sy_sem.at[i], ry_sem.at[i], (near, m)))
    for i, near in enumerate((mr, ml)):
        halos.append(remote(edge_s.at[i], edge_x.at[i], sx_sem.at[i], rx_sem.at[i], (g, near)))
    for copy in halos:
        copy.start()

    def find(i, carry):
        low = lax.rem(g + i + 1, n_grp) * span + m * slots
        index, mark = jnp.int32(0), jnp.int32(0)
        for s in range(slots):
            where_to = migrate_ref[s]
            hit = (where_to >= low) & (where_to < low + slots)
            index = jnp.where(hit, s, index)
            mark = jnp.where(hit, where_to - low + 1, mark)
        index_s[i] = index
        mark_s[i] = mark
        return carry

    lax.fori_loop(0, n_grp - 1, find, 0)

    load.wait()

    def slab(ref, level):
        start = level * slots
        if not isinstance(level, int):
            start = pl.multiple_of(start, slots)
        return ref[pl.ds(start, slots), :]

    def put(ref, level, value):
        start = level * slots
        if not isinstance(level, int):
            start = pl.multiple_of(start, slots)
        ref[pl.ds(start, slots), :] = value

    def clamp(level):
        if isinstance(level, int):
            return min(max(level, 0), levels - 1)
        return jnp.clip(level, 0, levels - 1)

    def explicit(ref, first, count):
        around = [slab(ref, clamp(first + j)) for j in range(-1, count + 1)]
        return [half_steps(around[j + 1], around[j + 2], around[j], width)
                for j in range(count)]

    def first_pass(first, count, carry):
        for j, value in enumerate(explicit(crm, first, count)):
            put(part, first + j, value)
        return carry

    blocks(levels, UNROLL, first_pass, 0)

    for copy in halos:
        copy.wait()

    position = lax.broadcasted_iota(jnp.int32, (points, LANES), 0)

    def sweep(value, before, after):
        lower = jnp.where(position == 0, before, pltpu.roll(value, 1, 0))
        upper = jnp.where(position == points - 1, after, pltpu.roll(value, points - 1, 0))
        return (value + jnp.where(position % 4 == 0, lower, 0.0)
                + jnp.where(position % 4 == 3, upper, 0.0))

    swept = [sweep(edge_y[0], edge_d[0, 0:1, :], edge_d[1, 0:1, :])]
    for r in range(rows):
        swept.append(sweep(values[r], edge_x[0, r:r + 1, :], edge_x[1, r:r + 1, :]))
    swept.append(sweep(edge_y[1], edge_d[2, 0:1, :], edge_d[3, 0:1, :]))
    results = []
    for r in range(rows):
        total = swept[r + 1]
        if r % 4 == 0:
            total = total + swept[r]
        if r % 4 == 3:
            total = total + swept[r + 2]
        result = total / total[:, fields:fields + 1]
        asm_ref[r] = result
        results.append(result)
    half = points // 2
    for b in range(rows // 2):
        pair[...] = 0.25 * (results[2 * b] + results[2 * b + 1])
        own_f[pl.ds(b * half, half), :] = (
            pair[pl.ds(0, half, stride=2), :] + pair[pl.ds(1, half, stride=2), :])

    sends = [
        remote(own_f, gathered.at[o - 1], sg_sem.at[o - 1], rg_sem.at[o - 1],
               (g, lax.rem(m + o, n_mem)))
        for o in range(1, n_mem)]
    for copy in sends:
        copy.start()
    column = lax.broadcasted_iota(jnp.int32, (slots, slots), 0)
    served = jnp.broadcast_to(bmap_ref[...], (slots, slots))

    def pick(source, rows_there):
        mine = (served == column + source * slots).astype(F32)
        return lax.dot_general(mine, rows_there, (((0,), (0,)), ((), ())),
                               precision=lax.Precision.HIGHEST, preferred_element_type=F32)

    count = jnp.broadcast_to(steps_ref[...].astype(F32), (LANES, slots)).T
    forcing = pick(m, own_f[...])
    for o in range(1, n_mem):
        sends[o - 1].wait()
        forcing = forcing + pick(lax.rem(m + n_mem - o, n_mem), gathered[o - 1])
    forcing = 0.25 * forcing

    lane_s = lax.broadcasted_iota(jnp.int32, (slots, LANES), 1)
    base = jnp.where(lane_s < width, 0, levels)

    def middle(first, number, carry):
        for j in range(number):
            force = jnp.take_along_axis(forcing, base + (first + j), axis=1)
            value = jnp.where(count > 0.5, slab(part, first + j) + force, slab(crm, first + j))
            put(mid, first + j, value)
            put(part, first + j, force)
        return carry

    blocks(levels, UNROLL, middle, 0)

    def leave(i, carry):
        target = lax.rem(g + i + 1, n_grp)
        at = pl.ds(index_s[i], levels, stride=slots)
        cur = mid[at, :]
        upper = jnp.concatenate([cur[1:], cur[-1:]], 0)
        lower = jnp.concatenate([cur[:1], cur[:-1]], 0)
        fresh = half_steps(cur, upper, lower, width) + part[at, :]
        twice = count_s[pl.ds(index_s[i], 1), :] > 1.5
        bucket[i, 0:levels, :] = jnp.where(twice, fresh, cur)
        bucket[i, levels:, :] = jnp.full((bucket.shape[1] - levels, LANES), mark_s[i].astype(F32))
        remote(bucket.at[i], arrived_ref.at[i], sb_sem.at[i], rb_sem.at[i], (target, m)).start()
        return carry

    count_s = tend
    count_s[...] = count
    if n_grp <= 8:
        for i in range(n_grp - 1):
            leave(i, 0)
    else:
        lax.fori_loop(0, n_grp - 1, leave, 0)

    def last(first, number, total):
        changes = []
        for j, fresh in enumerate(explicit(mid, first, number)):
            cur = jnp.where(count > 1.5, fresh + slab(part, first + j), slab(mid, first + j))
            put(stepped_ref, first + j, cur)
            changes.append(split(cur - slab(crm, first + j)))
        sums = jnp.dot(jnp.concatenate(changes, 0), same_ref[...], preferred_element_type=F32)
        for j in range(number):
            mine = lane_s - (first + j)
            mine = (mine == 0) | (mine == levels)
            total = jnp.where(mine, sums[j * slots:(j + 1) * slots], total)
        return total

    tendency = blocks(levels, UNROLL, last, jnp.zeros((slots, LANES), F32)) * (1.0 / width)

    def route(dest):
        mine = (served == column + dest * slots).astype(F32)
        return jnp.dot(mine, tendency, precision=lax.Precision.HIGHEST,
                       preferred_element_type=F32)

    returns = []
    for o in range(1, n_mem):
        dest = lax.rem(m + o, n_mem)
        outgoing[o - 1] = route(dest)
        copy = remote(outgoing.at[o - 1], incoming.at[o - 1], st_sem.at[o - 1], rt_sem.at[o - 1],
                      (g, dest))
        copy.start()
        returns.append(copy)
    sums = route(m)
    for o in range(1, n_mem):
        returns[o - 1].wait()
        sums = sums + incoming[o - 1]
    phys_ref[...] = sums

    def finish(i, carry):
        target = lax.rem(g + i + 1, n_grp)
        remote(bucket.at[i], arrived_ref.at[i], sb_sem.at[i], rb_sem.at[i], (target, m)).wait()
        return carry

    lax.fori_loop(0, n_grp - 1, finish, 0)


def place_outputs(n_grp, n_mem, levels, rows, points, slots, *refs):
    (migrate_ref, dyn_ref, asm_ref, phys_ref, stepped_ref, arrived_ref,
     dyn_out, phys_out, crm_out) = refs
    g = lax.axis_index("grp")
    span = n_mem * slots
    low = g * span
    for s in range(slots):
        where_to = migrate_ref[s]

        @pl.when((where_to >= low) & (where_to < low + span))
        def _():
            crm_out[pl.ds(lax.rem(where_to, slots), levels, stride=slots), :] = (
                stepped_ref[pl.ds(s, levels, stride=slots), :])

    for f in range(2):
        at = slice(f * levels, (f + 1) * levels)
        for r in range(rows):
            dyn_out[f, r] = dyn_ref[f, r] + 0.2 * asm_ref[r][:, at]
        phys_out[f] = phys_ref[...][:, at]

    def settle(i, carry):
        mark = jnp.max(arrived_ref[i, levels:levels + 1, :]).astype(jnp.int32)

        @pl.when(mark > 0)
        def _():
            crm_out[pl.ds(mark - 1, levels, stride=slots), :] = arrived_ref[i, 0:levels, :]

        return carry

    lax.fori_loop(0, n_grp - 1, settle, 0)


def on_device(n_grp, n_mem, dyn_state, wind_speed, mass_weight, crm_state, batch_map, sub_steps,
              migrate_to):
    _, levels, rows, points = dyn_state.shape
    slots = crm_state.shape[0]
    width = crm_state.shape[2] // 2
    fields = 2 * levels
    padded = levels // 8 * 8 + 8
    deriv = np.kron(np.eye(rows * points // 4), derivative_table()).astype(np.float32)
    k = np.arange(LANES)
    half_of_k = np.where(k < fields, k // levels, 2)
    half_of_x = np.arange(2 * width) // width
    same = np.tile((half_of_x[:, None] == half_of_k[None, :]).astype(np.float32), (2, 1))
    dyn2 = dyn_state.transpose(0, 2, 3, 1)
    wind2 = wind_speed.transpose(1, 2, 0)
    crm2 = crm_state.transpose(1, 0, 2).reshape(levels * slots, 2 * width)
    vmem = pl.BlockSpec(memory_space=pltpu.VMEM)
    smem = pl.BlockSpec(memory_space=pltpu.SMEM)
    hbm = pl.BlockSpec(memory_space=pl.ANY)
    dma = pltpu.SemaphoreType.DMA
    sds = jax.ShapeDtypeStruct
    buf = pltpu.VMEM
    asm, phys, stepped, arrived = pl.pallas_call(
        functools.partial(exchange, n_grp, n_mem, levels, rows, points, slots, width),
        out_shape=(
            sds((rows, points, LANES), F32),
            sds((slots, LANES), F32),
            sds((levels * slots, 2 * width), F32),
            sds((n_grp - 1, padded, LANES), F32),
        ),
        in_specs=[vmem, vmem, vmem, hbm, vmem, vmem, smem, vmem, vmem],
        out_specs=(vmem, vmem, vmem, hbm),
        scratch_shapes=[
            buf((levels * slots, 2 * width), F32),
            buf((levels * slots, 2 * width), F32),
            buf((levels * slots, 2 * width), F32),
            buf((rows * points, LANES), F32),
            buf((rows * points, LANES), F32),
            buf((2, 8, LANES), F32),
            buf((2, 8, LANES), F32),
            buf((2, points, LANES), F32),
            buf((2, points, LANES), F32),
            buf((4, 8, LANES), F32),
            buf((4, 8, LANES), F32),
            buf((points, LANES), F32),
            buf((slots, LANES), F32),
            buf((n_mem - 1, slots, LANES), F32),
            buf((n_grp - 1, padded, LANES), F32),
            buf((slots, LANES), F32),
            buf((n_mem - 1, slots, LANES), F32),
            buf((n_mem - 1, slots, LANES), F32),
            pltpu.SMEM((n_grp,), jnp.int32),
            pltpu.SMEM((n_grp,), jnp.int32),
            dma,
            dma((2,)), dma((2,)), dma((2,)), dma((2,)), dma((4,)), dma((4,)),
            dma((n_mem - 1,)), dma((n_mem - 1,)),
            dma((n_grp - 1,)), dma((n_grp - 1,)),
            dma((n_mem - 1,)), dma((n_mem - 1,)),
        ],
        compiler_params=pltpu.CompilerParams(collective_id=0, has_side_effects=True),
        name="exchange",
    )(dyn2, wind2, mass_weight, crm2, batch_map[None, :], sub_steps[None, :], migrate_to,
      jnp.asarray(deriv), jnp.asarray(same).astype(BF16))
    dyn_next, phys_tend, crm_next = pl.pallas_call(
        functools.partial(place_outputs, n_grp, n_mem, levels, rows, points, slots),
        out_shape=(
            sds(dyn2.shape, F32),
            sds((2, slots, levels), F32),
            sds((levels * slots, 2 * width), F32),
        ),
        in_specs=[smem, vmem, vmem, vmem, vmem, vmem],
        out_specs=(vmem, vmem, vmem),
        name="place",
    )(migrate_to, dyn2, asm, phys, stepped, arrived)
    crm_next = crm_next.reshape(levels, slots, 2 * width).transpose(1, 0, 2)
    return dyn_next.transpose(0, 3, 1, 2), phys_tend.transpose(0, 2, 1), crm_next


def solution(mesh):
    n_grp, n_mem = mesh.shape["grp"], mesh.shape["mem"]
    grid = P(None, None, "grp", "mem")
    slot = P(("grp", "mem"))
    return jax.shard_map(
        functools.partial(on_device, n_grp, n_mem),
        mesh=mesh,
        in_specs=(grid, P(None, "grp", "mem"), P("grp", "mem"), P(("grp", "mem"), None, None),
                  slot, slot, slot),
        out_specs=(grid, P(None, None, ("grp", "mem")), P(("grp", "mem"), None, None)),
        check_vma=False,
    )
```

```python
import functools

import jax
import jax.numpy as jnp
import numpy as np
from jax import lax
from jax.experimental import pallas as pl
from jax.experimental.pallas import tpu as pltpu
from jax.sharding import PartitionSpec as P

NSUB = 2
MESH = pl.DeviceIdType.MESH
F32 = jnp.float32
BF16 = jnp.bfloat16
LANES = 128
UNROLL = 8
CHUNK = 16


def derivative_table():
    nodes = np.array([-1.0, -1.0 / np.sqrt(5.0), 1.0 / np.sqrt(5.0), 1.0])
    table = np.zeros((4, 4))
    for i in range(4):
        for j in range(4):
            if i == j:
                table[i, j] = sum(1.0 / (nodes[j] - nodes[o]) for o in range(4) if o != j)
            else:
                top, bottom = 1.0, 1.0
                for o in range(4):
                    if o != j and o != i:
                        top = top * (nodes[i] - nodes[o])
                    if o != j:
                        bottom = bottom * (nodes[j] - nodes[o])
                table[i, j] = top / bottom
    return table.astype(np.float32)


def split(values):
    high = values.astype(BF16)
    low = (values - high.astype(F32)).astype(BF16)
    return jnp.concatenate([high, low], axis=-1)


def half_steps(cur, upper, lower, width):
    lane = lax.broadcasted_iota(jnp.int32, cur.shape, 1)
    heat = lane < width
    inner = lane % width
    other = pltpu.roll(cur, width, 1)
    diff = other - cur
    gap = jnp.where(heat, diff, -diff)
    condense = jnp.maximum(gap, 0.0) + jnp.log(1.0 + jnp.exp(-jnp.abs(gap)))
    left = jnp.where(inner == 0, pltpu.roll(cur, width + 1, 1), pltpu.roll(cur, 1, 1))
    right = jnp.where(
        inner == width - 1,
        pltpu.roll(cur, width - 1, 1),
        pltpu.roll(cur, 2 * width - 1, 1),
    )
    scale = jnp.where(heat, 0.05, -0.1)
    return 0.5 * cur + 0.15 * (left + right) + 0.1 * (upper + lower) + scale * condense


def blocks(levels, unroll, body, carry):
    full = levels // unroll
    if full:
        carry = lax.fori_loop(0, full, lambda i, c: body(i * unroll, unroll, c), carry)
    if levels % unroll:
        carry = body(full * unroll, levels % unroll, carry)
    return carry


def exchange(n_grp, n_mem, levels, rows, points, slots, width, *refs):
    (dyn_hbm, wind_hbm, mass_hbm, crm_hbm, bmap_hbm, steps_hbm, migrate_hbm,
     deriv_hbm, same_hbm,
     asm_hbm, phys_ref, stepped_hbm, arrived_ref,
     dyn_ref, wind_ref, mass_ref, bmap_ref, steps_ref, migrate_ref, deriv_ref, same_ref, asm_ref,
     crm, part, mid, xs, ws, edge_s, edge_x, edge_y_s, edge_y, edge_d_s, edge_d,
     pair, own_f, gathered, bucket, tend, outgoing, incoming, index_s, mark_s,
     crm_sem, in_sem, asm_sem, out_sem, sx_sem, rx_sem, sy_sem, ry_sem, sd_sem, rd_sem,
     sg_sem, rg_sem, sb_sem, rb_sem, st_sem, rt_sem) = refs
    g, m = lax.axis_index("grp"), lax.axis_index("mem")
    fields = 2 * levels
    span = n_mem * slots

    gu, gd = lax.rem(g + n_grp - 1, n_grp), lax.rem(g + 1, n_grp)
    ml, mr = lax.rem(m + n_mem - 1, n_mem), lax.rem(m + 1, n_mem)
    corners = ((gd, mr), (gd, ml), (gu, mr), (gu, ml))
    barrier = pltpu.get_barrier_semaphore()
    for o in range(1, n_grp):
        pl.semaphore_signal(barrier, 1, device_id=(lax.rem(g + o, n_grp), m), device_id_type=MESH)
    for o in range(1, n_mem):
        pl.semaphore_signal(barrier, 1, device_id=(g, lax.rem(m + o, n_mem)), device_id_type=MESH)
    for corner in corners:
        pl.semaphore_signal(barrier, 1, device_id=corner, device_id_type=MESH)

    pairs = ((dyn_hbm, dyn_ref), (deriv_hbm, deriv_ref), (wind_hbm, wind_ref),
             (mass_hbm, mass_ref), (migrate_hbm, migrate_ref), (bmap_hbm, bmap_ref),
             (steps_hbm, steps_ref), (same_hbm, same_ref))
    loads = [pltpu.make_async_copy(a, b, in_sem.at[i]) for i, (a, b) in enumerate(pairs)]
    for copy in loads:
        copy.start()
    load = pltpu.make_async_copy(crm_hbm, crm, crm_sem)
    load.start()
    for copy in loads:
        copy.wait()

    for r in range(rows):
        at = pl.ds(r * points, points)
        for f in range(2):
            xs[at, f * levels:(f + 1) * levels] = dyn_ref[f, r]
            ws[at, f * levels:(f + 1) * levels] = wind_ref[r]
        spread_mass = jnp.broadcast_to(mass_ref[r:r + 1, :], (LANES, points)).T
        xs[at, fields:] = jnp.zeros((points, LANES - fields), F32)
        ws[at, fields:] = -spread_mass[:, fields:]
    lane = lax.broadcasted_iota(jnp.int32, (points, LANES), 1)
    values = []
    dx = jnp.dot(deriv_ref[...], xs[...], precision=lax.Precision.HIGHEST,
                 preferred_element_type=F32)
    for r in range(rows):
        at = slice(r * points, (r + 1) * points)
        spread_mass = jnp.broadcast_to(mass_ref[r:r + 1, :], (LANES, points)).T
        advected = -ws[at] * jnp.where(lane < fields, dx[at] * spread_mass, 1.0)
        values.append(advected)
        edge_s[0, r:r + 1, :] = advected[points - 1:, :]
        edge_s[1, r:r + 1, :] = advected[:1, :]
        if r == rows - 1:
            edge_y_s[0] = advected
            edge_d_s[0, 0:1, :] = advected[points - 1:, :]
            edge_d_s[1, 0:1, :] = advected[:1, :]
        if r == 0:
            edge_y_s[1] = advected
            edge_d_s[2, 0:1, :] = advected[points - 1:, :]
            edge_d_s[3, 0:1, :] = advected[:1, :]

    pl.semaphore_wait(barrier, n_grp - 1 + n_mem - 1 + 4)

    def remote(src, dst, ssem, rsem, device):
        return pltpu.make_async_remote_copy(
            src_ref=src, dst_ref=dst, send_sem=ssem, recv_sem=rsem,
            device_id=device, device_id_type=MESH)

    halos = []
    for i, corner in enumerate(corners):
        halos.append(remote(edge_d_s.at[i], edge_d.at[i], sd_sem.at[i], rd_sem.at[i], corner))
    for i, near in enumerate((gd, gu)):
        halos.append(remote(edge_y_s.at[i], edge_y.at[i], sy_sem.at[i], ry_sem.at[i], (near, m)))
    for i, near in enumerate((mr, ml)):
        halos.append(remote(edge_s.at[i], edge_x.at[i], sx_sem.at[i], rx_sem.at[i], (g, near)))
    for copy in halos:
        copy.start()

    def find(i, carry):
        low = lax.rem(g + i + 1, n_grp) * span + m * slots
        index, mark = jnp.int32(0), jnp.int32(0)
        for s in range(slots):
            where_to = migrate_ref[s]
            hit = (where_to >= low) & (where_to < low + slots)
            index = jnp.where(hit, s, index)
            mark = jnp.where(hit, where_to - low + 1, mark)
        index_s[i] = index
        mark_s[i] = mark
        return carry

    lax.fori_loop(0, n_grp - 1, find, 0)

    load.wait()

    stride = slots + 8

    def rows_of(ref, level):
        step = slots if ref is crm else stride
        start = level * step
        if not isinstance(level, int):
            start = pl.multiple_of(start, 8)
        return pl.ds(start, slots)

    def slab(ref, level):
        return ref[rows_of(ref, level), :]

    def put(ref, level, value):
        ref[rows_of(ref, level), :] = value

    def clamp(level):
        if isinstance(level, int):
            return min(max(level, 0), levels - 1)
        return jnp.clip(level, 0, levels - 1)

    def explicit(ref, first, count):
        around = [slab(ref, clamp(first + j)) for j in range(-1, count + 1)]
        return [half_steps(around[j + 1], around[j + 2], around[j], width)
                for j in range(count)]

    def first_pass(first, count, carry):
        for j, value in enumerate(explicit(crm, first, count)):
            put(part, first + j, value)
        return carry

    blocks(levels, UNROLL, first_pass, 0)

    for copy in halos:
        copy.wait()

    position = lax.broadcasted_iota(jnp.int32, (points, LANES), 0)

    def sweep(value, before, after):
        lower = jnp.where(position == 0, before, pltpu.roll(value, 1, 0))
        upper = jnp.where(position == points - 1, after, pltpu.roll(value, points - 1, 0))
        return (value + jnp.where(position % 4 == 0, lower, 0.0)
                + jnp.where(position % 4 == 3, upper, 0.0))

    swept = [sweep(edge_y[0], edge_d[0, 0:1, :], edge_d[1, 0:1, :])]
    for r in range(rows):
        swept.append(sweep(values[r], edge_x[0, r:r + 1, :], edge_x[1, r:r + 1, :]))
    swept.append(sweep(edge_y[1], edge_d[2, 0:1, :], edge_d[3, 0:1, :]))
    results = []
    for r in range(rows):
        total = swept[r + 1]
        if r % 4 == 0:
            total = total + swept[r]
        if r % 4 == 3:
            total = total + swept[r + 2]
        result = total / total[:, fields:fields + 1]
        asm_ref[r] = result
        results.append(result)
    asm_copy = pltpu.make_async_copy(asm_ref, asm_hbm, asm_sem)
    half = points // 2
    for b in range(rows // 2):
        pair[...] = 0.25 * (results[2 * b] + results[2 * b + 1])
        own_f[pl.ds(b * half, half), :] = (
            pair[pl.ds(0, half, stride=2), :] + pair[pl.ds(1, half, stride=2), :])

    sends = [
        remote(own_f, gathered.at[o - 1], sg_sem.at[o - 1], rg_sem.at[o - 1],
               (g, lax.rem(m + o, n_mem)))
        for o in range(1, n_mem)]
    for copy in sends:
        copy.start()
    asm_copy.start()
    column = lax.broadcasted_iota(jnp.int32, (slots, slots), 0)
    served = jnp.broadcast_to(bmap_ref[...], (slots, slots))

    origins = [m] + [lax.rem(m + n_mem - o, n_mem) for o in range(1, n_mem)]
    mine = jnp.concatenate([served == column + at * slots for at in origins], 0).astype(F32).T
    count = jnp.broadcast_to(steps_ref[...].astype(F32), (LANES, slots)).T
    for copy in sends:
        copy.wait()
    everyone = jnp.concatenate([own_f[...]] + [gathered[o] for o in range(n_mem - 1)], 0)
    forcing = 0.25 * jnp.dot(mine, everyone, precision=lax.Precision.HIGHEST,
                             preferred_element_type=F32)

    lane_s = lax.broadcasted_iota(jnp.int32, (slots, LANES), 1)
    base = jnp.where(lane_s < width, 0, levels)

    def middle(first, number, carry):
        for j in range(number):
            force = jnp.take_along_axis(forcing, base + (first + j), axis=1)
            value = jnp.where(count > 0.5, slab(part, first + j) + force, slab(crm, first + j))
            put(mid, first + j, value)
            put(part, first + j, force)
        return carry

    blocks(levels, UNROLL, middle, 0)

    def leave(i, carry):
        target = lax.rem(g + i + 1, n_grp)
        at = pl.ds(index_s[i], levels, stride=stride)
        cur = mid[at, :]
        upper = jnp.concatenate([cur[1:], cur[-1:]], 0)
        lower = jnp.concatenate([cur[:1], cur[:-1]], 0)
        fresh = half_steps(cur, upper, lower, width) + part[at, :]
        twice = count_s[pl.ds(index_s[i], 1), :] > 1.5
        bucket[i, 0:levels, :] = jnp.where(twice, fresh, cur)
        bucket[i, levels:, :] = jnp.full((bucket.shape[1] - levels, LANES), mark_s[i].astype(F32))
        remote(bucket.at[i], arrived_ref.at[i], sb_sem.at[i], rb_sem.at[i], (target, m)).start()
        return carry

    count_s = tend
    count_s[...] = count
    if n_grp <= 8:
        for i in range(n_grp - 1):
            leave(i, 0)
    else:
        lax.fori_loop(0, n_grp - 1, leave, 0)

    def drain(first, number):
        start = first * slots
        if not isinstance(first, int):
            start = pl.multiple_of(start, slots)
        at = pl.ds(start, number * slots)
        return pltpu.make_async_copy(crm.at[at], stepped_hbm.at[at], out_sem.at[first // UNROLL])

    def last(first, number, total):
        changes = []
        for j, fresh in enumerate(explicit(mid, first, number)):
            cur = jnp.where(count > 1.5, fresh + slab(part, first + j), slab(mid, first + j))
            changes.append(split(cur - slab(crm, first + j)))
            put(crm, first + j, cur)
        drain(first, number).start()
        sums = jnp.dot(jnp.concatenate(changes, 0), same_ref[...], preferred_element_type=F32)
        for j in range(number):
            mine = lane_s - (first + j)
            mine = (mine == 0) | (mine == levels)
            total = jnp.where(mine, sums[j * slots:(j + 1) * slots], total)
        return total

    tendency = blocks(levels, UNROLL, last, jnp.zeros((slots, LANES), F32)) * (1.0 / width)

    def route(dest):
        mine = (served == column + dest * slots).astype(F32)
        return jnp.dot(mine, tendency, precision=lax.Precision.HIGHEST,
                       preferred_element_type=F32)

    returns = []
    for o in range(1, n_mem):
        dest = lax.rem(m + o, n_mem)
        outgoing[o - 1] = route(dest)
        copy = remote(outgoing.at[o - 1], incoming.at[o - 1], st_sem.at[o - 1], rt_sem.at[o - 1],
                      (g, dest))
        copy.start()
        returns.append(copy)
    sums = route(m)
    for o in range(1, n_mem):
        returns[o - 1].wait()
        sums = sums + incoming[o - 1]
    phys_ref[...] = sums

    def drained(first, number, carry):
        drain(first, number).wait()
        return carry

    blocks(levels, UNROLL, drained, 0)
    asm_copy.wait()

    def finish(i, carry):
        target = lax.rem(g + i + 1, n_grp)
        remote(bucket.at[i], arrived_ref.at[i], sb_sem.at[i], rb_sem.at[i], (target, m)).wait()
        return carry

    lax.fori_loop(0, n_grp - 1, finish, 0)


def place_outputs(n_grp, n_mem, levels, rows, points, slots, *refs):
    (migrate_ref, dyn_ref, asm_ref, phys_ref, stepped_hbm, arrived_ref,
     dyn_out, phys_out, crm_hbm, pool, placed, in_sem, out_sem) = refs
    g = lax.axis_index("grp")
    span = n_mem * slots
    low = g * span
    stride = slots + 8
    chunks = [(c, min(CHUNK, levels - c)) for c in range(0, levels, CHUNK)]
    loads, stores = [], []
    for i, (start, size) in enumerate(chunks):
        levels_at, slots_at = pl.ds(start, size), pl.ds(0, slots)
        loads.append(pltpu.make_async_copy(
            stepped_hbm.at[levels_at], pool.at[levels_at, slots_at], in_sem.at[i]))
        stores.append(pltpu.make_async_copy(
            placed.at[levels_at, slots_at], crm_hbm.at[levels_at], out_sem.at[i]))
    for copy in loads:
        copy.start()
    for f in range(2):
        at = slice(f * levels, (f + 1) * levels)
        for r in range(rows):
            dyn_out[f, r] = dyn_ref[f, r] + 0.2 * asm_ref[r][:, at]
        phys_out[f] = phys_ref[...][:, at]
    targets = []
    for s in range(slots):
        where_to = migrate_ref[s]
        staying = (where_to >= low) & (where_to < low + span)
        targets.append(jnp.where(staying, lax.rem(where_to, slots), slots))
    flat_pool = pool.reshape(levels * stride, pool.shape[2])
    flat_placed = placed.reshape(levels * stride, pool.shape[2])

    def landing(i):
        mark = jnp.max(arrived_ref[i, levels:levels + 1, :]).astype(jnp.int32)
        return jnp.where(mark > 0, mark - 1, slots)

    few = n_grp <= 8
    if few:
        landings = [landing(i) for i in range(n_grp - 1)]
    for i, (start, size) in enumerate(chunks):
        loads[i].wait()
        first = start * stride
        for s in range(slots):
            flat_placed[pl.ds(first + targets[s], size, stride=stride), :] = (
                flat_pool[pl.ds(first + s, size, stride=stride), :])

        def settle(j, carry):
            target = landings[j] if few else landing(j)
            flat_placed[pl.ds(first + target, size, stride=stride), :] = (
                arrived_ref[j, start:start + size, :])
            return carry

        if few:
            for j in range(n_grp - 1):
                settle(j, 0)
        else:
            lax.fori_loop(0, n_grp - 1, settle, 0)
        stores[i].start()
    for copy in stores:
        copy.wait()


def on_device(n_grp, n_mem, dyn_state, wind_speed, mass_weight, crm_state, batch_map, sub_steps,
              migrate_to):
    _, levels, rows, points = dyn_state.shape
    slots = crm_state.shape[0]
    width = crm_state.shape[2] // 2
    fields = 2 * levels
    padded = levels // 8 * 8 + 8
    deriv = np.kron(np.eye(rows * points // 4), derivative_table()).astype(np.float32)
    k = np.arange(LANES)
    half_of_k = np.where(k < fields, k // levels, 2)
    half_of_x = np.arange(2 * width) // width
    same = np.tile((half_of_x[:, None] == half_of_k[None, :]).astype(np.float32), (2, 1))
    dyn2 = dyn_state.transpose(0, 2, 3, 1)
    wind2 = wind_speed.transpose(1, 2, 0)
    crm2 = crm_state.transpose(1, 0, 2).reshape(levels * slots, 2 * width)
    vmem = pl.BlockSpec(memory_space=pltpu.VMEM)
    smem = pl.BlockSpec(memory_space=pltpu.SMEM)
    hbm = pl.BlockSpec(memory_space=pl.ANY)
    dma = pltpu.SemaphoreType.DMA
    sds = jax.ShapeDtypeStruct
    buf = pltpu.VMEM
    asm, phys, stepped, arrived = pl.pallas_call(
        functools.partial(exchange, n_grp, n_mem, levels, rows, points, slots, width),
        out_shape=(
            sds((rows, points, LANES), F32),
            sds((slots, LANES), F32),
            sds((levels * slots, 2 * width), F32),
            sds((n_grp - 1, padded, LANES), F32),
        ),
        in_specs=[hbm] * 9,
        out_specs=(hbm, vmem, hbm, hbm),
        scratch_shapes=[
            buf(dyn2.shape, F32),
            buf(wind2.shape, F32),
            buf((rows, points), F32),
            buf((1, slots), jnp.int32),
            buf((1, slots), jnp.int32),
            pltpu.SMEM((slots,), jnp.int32),
            buf(deriv.shape, F32),
            buf(same.shape, BF16),
            buf((rows, points, LANES), F32),
            buf((levels * slots, 2 * width), F32),
            buf((levels * (slots + 8), 2 * width), F32),
            buf((levels * (slots + 8), 2 * width), F32),
            buf((rows * points, LANES), F32),
            buf((rows * points, LANES), F32),
            buf((2, 8, LANES), F32),
            buf((2, 8, LANES), F32),
            buf((2, points, LANES), F32),
            buf((2, points, LANES), F32),
            buf((4, 8, LANES), F32),
            buf((4, 8, LANES), F32),
            buf((points, LANES), F32),
            buf((slots, LANES), F32),
            buf((n_mem - 1, slots, LANES), F32),
            buf((n_grp - 1, padded, LANES), F32),
            buf((slots, LANES), F32),
            buf((n_mem - 1, slots, LANES), F32),
            buf((n_mem - 1, slots, LANES), F32),
            pltpu.SMEM((n_grp,), jnp.int32),
            pltpu.SMEM((n_grp,), jnp.int32),
            dma, dma((8,)), dma, dma((levels // UNROLL + 1,)),
            dma((2,)), dma((2,)), dma((2,)), dma((2,)), dma((4,)), dma((4,)),
            dma((n_mem - 1,)), dma((n_mem - 1,)),
            dma((n_grp - 1,)), dma((n_grp - 1,)),
            dma((n_mem - 1,)), dma((n_mem - 1,)),
        ],
        compiler_params=pltpu.CompilerParams(collective_id=0, has_side_effects=True),
        name="exchange",
    )(dyn2, wind2, mass_weight, crm2, batch_map[None, :], sub_steps[None, :], migrate_to,
      jnp.asarray(deriv), jnp.asarray(same).astype(BF16))
    dyn_next, phys_tend, crm_next = pl.pallas_call(
        functools.partial(place_outputs, n_grp, n_mem, levels, rows, points, slots),
        out_shape=(
            sds(dyn2.shape, F32),
            sds((2, slots, levels), F32),
            sds((levels, slots, 2 * width), F32),
        ),
        in_specs=[smem, vmem, vmem, vmem, hbm, vmem],
        out_specs=(vmem, vmem, hbm),
        scratch_shapes=[
            buf((levels, slots + 8, 2 * width), F32),
            buf((levels, slots + 8, 2 * width), F32),
            dma((levels // CHUNK + 1,)), dma((levels // CHUNK + 1,)),
        ],
        name="place",
    )(migrate_to, dyn2, asm, phys, stepped.reshape(levels, slots, 2 * width), arrived)
    crm_next = crm_next.transpose(1, 0, 2)
    return dyn_next.transpose(0, 3, 1, 2), phys_tend.transpose(0, 2, 1), crm_next


def solution(mesh):
    n_grp, n_mem = mesh.shape["grp"], mesh.shape["mem"]
    grid = P(None, None, "grp", "mem")
    slot = P(("grp", "mem"))
    return jax.shard_map(
        functools.partial(on_device, n_grp, n_mem),
        mesh=mesh,
        in_specs=(grid, P(None, "grp", "mem"), P("grp", "mem"), P(("grp", "mem"), None, None),
                  slot, slot, slot),
        out_specs=(grid, P(None, None, ("grp", "mem")), P(("grp", "mem"), None, None)),
        check_vma=False,
    )
```
